32 devices in a mesh: row: 8 (over z, core), col: 4 (over y, x).
Axes of the slice: x: 2, y: 2, z: 4, core: 2. Of those that a mesh axis runs over, the one named last changes fastest.
Arguments:
- inverse_tiles: bfloat16 [12288, 12288], P('row', 'col'), may hold values from -6 to 6
- factor: bfloat16 [12288, 2048], P('row', 'col'), may hold values from -0.0546875 to 0.0546875
- block_mask: int32 [96, 16], replicated, may hold values 0 or 1
- diag_inverse: float32 [16, 128, 128], replicated, may hold values from -6 to 6
Outputs:
- off_block: bfloat16 [2048, 12288], P('col', 'row')
- diag_block: float32 [16, 128, 128], P('col')
The draws below stay inside these ranges and needn't reach their ends.
All inputs are finite; a program needn't handle non-finite values.
Results may differ from the reference program's by a relative error of at most 0.012.
Values may be sent and summed in bfloat16 or wider, within the bound.
No kernel may reach another device: no remote copies, remote signals or barrier semaphores. Data moves between devices by JAX's collectives and lax.ppermute only.
A program may use at most 128 MiB of HBM per device.

```python
import jax
import jax.numpy as jnp
from jax import lax

W = 128
NSUP = 16
R = 12288
NB = 96


def plant(array, key, least, top_value):
    place = [jax.random.randint(jax.random.fold_in(key, axis), (), 0, length) for axis, length in enumerate(array.shape)]
    widest = array.shape.index(max(array.shape))
    neighbour = place[:widest] + [(place[widest] + 1) % array.shape[widest]] + place[widest + 1:]
    return array.at[tuple(place)].set(least).at[tuple(neighbour)].set(top_value)


def shard_levels(stream_key, extent, shards, low, top_value):
    factor_of, own = 1.0, jax.random.fold_in(stream_key, 6)
    for position, shards_of in shards:
        steps = jnp.exp(jax.random.uniform(jax.random.fold_in(own, position), (shards_of,), jnp.float32, low / len(shards), top_value / len(shards)))
        factor_of = factor_of * jnp.repeat(steps, extent[position] // shards_of).reshape([-1 if axis == position else 1 for axis in range(len(extent))])
    return factor_of


def scatter_about(key, dims, deviation, limit, pieces=(), kind=jnp.bfloat16):
    level = shard_levels(key, dims, pieces, -0.22, 0.18) if pieces else 1.0
    drawn = jax.random.normal(key, dims, jnp.float32) * deviation * level
    return jnp.minimum(jnp.maximum(drawn, -limit), limit).astype(kind)


def setup_inputs(seed: int = 0) -> dict:
    key_of = jax.random.split(jax.random.key(seed), 5)
    inverse_tiles = scatter_about(key_of[0], (R, R), 1.0, 6.0, ((0, 8), (1, 4)))
    factor = scatter_about(key_of[1], (R, NSUP * W), R ** -0.5, 0.0546875, ((0, 8), (1, 4)))
    block_mask = plant((jax.random.randint(key_of[2], (NB, NSUP), 0, 5) < 4).astype(jnp.int32), jax.random.fold_in(key_of[2], 1), 0, 1)
    diag_inverse = scatter_about(key_of[3], (NSUP, W, W), 1.0, 6.0, (), jnp.float32)
    return {"inverse_tiles": inverse_tiles, "factor": factor, "block_mask": block_mask, "diag_inverse": diag_inverse}


def reference(inverse_tiles, factor, block_mask, diag_inverse):
    keep_mask = jnp.repeat(jnp.repeat(block_mask, W, 0), W, 1).astype(jnp.bfloat16)
    masked = factor * keep_mask
    product = jnp.dot(inverse_tiles, masked, preferred_element_type=jnp.float32)
    off_block = (-product).T.astype(jnp.bfloat16)
    left_factor = masked.astype(jnp.float32).reshape(-1, NSUP, W)
    right_product = product.reshape(-1, NSUP, W)
    diag_block = diag_inverse + jnp.einsum("rja,rjb->jab", left_factor, right_product, precision=lax.Precision.HIGHEST)
    return off_block, diag_block
```

```python
import jax
import jax.numpy as jnp
from jax import lax
from jax.sharding import PartitionSpec as P


AXES = ("row", "col")


def bf16(value):
    return lax.reduce_precision(value, 8, 7).astype(jnp.bfloat16)


def body(inverse_tiles, factor, block_mask, diag_inverse):
    rows_here, cols_here = factor.shape
    width = diag_inverse.shape[1]
    sup_here = cols_here // width
    blocks_here = rows_here // width
    n_row, n_col = lax.axis_size("row"), lax.axis_size("col")
    ratio = n_row // n_col
    row_index = lax.axis_index("row")
    col_index = lax.axis_index("col")
    plane, part = row_index // ratio, row_index % ratio

    def send(value, target):
        pairs = []
        for row in range(n_row):
            for col in range(n_col):
                to_row, to_col = target(row, col)
                pairs.append((row * n_col + col, to_row * n_col + to_col))
        return lax.ppermute(value, AXES, pairs)

    def spread(step):
        return lambda row, col: ((col ^ step) * ratio + row % ratio, row // ratio)

    def swap(step):
        return lambda row, col: (row // ratio * ratio + (row + step) % ratio, col)

    def shift(step):
        return lambda row, col: (row, col ^ step)

    def flip(step):
        return lambda row, col: ((row // ratio ^ step) * ratio + row % ratio, col)

    mask_here = lax.dynamic_slice(
        block_mask, (row_index * blocks_here, col_index * sup_here), (blocks_here, sup_here)
    ).astype(jnp.bfloat16)
    blocks = factor.reshape(blocks_here, width, cols_here)

    own, gathered = [], []
    chunks = split(sup_here)
    for low, high in chunks:
        piece = blocks[:, :, low * width : high * width]
        keep = jnp.repeat(mask_here[:, low:high], width, 1)
        piece = (piece * keep[:, None, :]).reshape(rows_here, -1)
        own.append(piece)
        gathered.append([send(piece, spread(step)) for step in range(n_col)])

    parts = [
        lax.dynamic_slice_in_dim(inverse_tiles, (part + ratio - step) % ratio * rows_here, rows_here, 1)
        for step in range(ratio)
    ]

    def exchange(partial):
        partial = bf16(partial)
        pair = partial.astype(jnp.float32)
        for step in range(1, ratio):
            pair = pair + send(partial, swap(step)).astype(jnp.float32)
        pair = bf16(pair)
        terms = [pair] + [send(pair, flip(step)) for step in range(1, n_col)]
        terms = [t.astype(jnp.float32) for t in terms]
        while len(terms) > 1:
            terms = [terms[i] + terms[i + 1] for i in range(0, len(terms), 2)]
        return terms[0]

    own_diag = lax.dynamic_slice_in_dim(diag_inverse, col_index * sup_here, sup_here, 0)
    diag, off = [], []
    for chunk, (low, high) in enumerate(chunks):
        product = None
        for step in range(ratio):
            got = gathered[chunk]
            if step:
                got = [send(g, swap(step)) for g in got]
            term = lax.dot_general(
                jnp.concatenate(got, axis=1),
                parts[step],
                (((0,), (1,)), ((), ())),
                preferred_element_type=jnp.float32,
            )
            product = term if product is None else product + term
        product = product.reshape(n_col, -1, rows_here)
        slots = []
        for step in range(n_col):
            slots.append(
                lax.dynamic_index_in_dim(product, plane ^ col_index ^ step, 0, keepdims=False)
            )
        arrived = [send(slots[step].astype(jnp.bfloat16), shift(step)) for step in range(1, n_col)]
        total = slots[0]
        for value in arrived:
            total = total + value.astype(jnp.float32)
        off.append((-total).astype(jnp.bfloat16))
        low_total = total.astype(jnp.bfloat16)
        for sup in range(high - low):
            part_of = slice(sup * width, (sup + 1) * width)
            diag.append(
                lax.dot_general(
                    own[chunk][:, part_of],
                    low_total[part_of],
                    (((0,), (1,)), ((), ())),
                    preferred_element_type=jnp.float32,
                )
            )
    sums = []
    last = chunks[-1][0]
    if last:
        sums.append(exchange(jnp.stack(diag[:last])))
    sums.append(exchange(jnp.stack(diag[last:])))
    return jnp.concatenate(off, axis=0), own_diag + jnp.concatenate(sums)


def split(count):
    edges = list(range(count + 1))
    return list(zip(edges[:-1], edges[1:]))


def solution(mesh):
    return jax.shard_map(
        body,
        mesh=mesh,
        in_specs=(P("row", "col"), P("row", "col"), P(), P()),
        out_specs=(P("col", "row"), P("col", None, None)),
        check_vma=False,
    )
```

```python
import jax
import jax.numpy as jnp
from jax import lax
from jax.sharding import PartitionSpec as P


AXES = ("row", "col")


def bf16(value):
    return lax.reduce_precision(value, 8, 7).astype(jnp.bfloat16)


def body(inverse_tiles, factor, block_mask, diag_inverse):
    rows_here, cols_here = factor.shape
    width = diag_inverse.shape[1]
    sup_here = cols_here // width
    blocks_here = rows_here // width
    n_row, n_col = lax.axis_size("row"), lax.axis_size("col")
    ratio = n_row // n_col
    row_index = lax.axis_index("row")
    col_index = lax.axis_index("col")
    plane, part = row_index // ratio, row_index % ratio

    def send(value, target):
        pairs = []
        for row in range(n_row):
            for col in range(n_col):
                to_row, to_col = target(row, col)
                pairs.append((row * n_col + col, to_row * n_col + to_col))
        return lax.ppermute(value, AXES, pairs)

    def spread(step):
        return lambda row, col: ((col ^ step) * ratio + row % ratio, row // ratio)

    def swap(step):
        return lambda row, col: (row // ratio * ratio + (row + step) % ratio, col)

    def shift(step):
        return lambda row, col: (row, col ^ step)

    def flip(step):
        return lambda row, col: ((row // ratio ^ step) * ratio + row % ratio, col)

    mask_here = lax.dynamic_slice(
        block_mask, (row_index * blocks_here, col_index * sup_here), (blocks_here, sup_here)
    ).astype(jnp.bfloat16)
    blocks = factor.reshape(blocks_here, width, cols_here)

    own, gathered = [], []
    chunks = split(sup_here)
    for low, high in chunks:
        piece = blocks[:, :, low * width : high * width]
        keep = jnp.repeat(mask_here[:, low:high], width, 1)
        piece = (piece * keep[:, None, :]).reshape(rows_here, -1)
        own.append(piece)
        gathered.append([send(piece, spread(step)) for step in range(n_col)])

    parts = [
        lax.dynamic_slice_in_dim(inverse_tiles, (part + ratio - step) % ratio * rows_here, rows_here, 1)
        for step in range(ratio)
    ]

    def exchange(partial):
        partial = bf16(partial)
        pair = partial.astype(jnp.float32)
        for step in range(1, ratio):
            pair = pair + send(partial, swap(step)).astype(jnp.float32)
        pair = bf16(pair)
        terms = [pair] + [send(pair, flip(step)) for step in range(1, n_col)]
        terms = [t.astype(jnp.float32) for t in terms]
        while len(terms) > 1:
            terms = [terms[i] + terms[i + 1] for i in range(0, len(terms), 2)]
        return terms[0]

    own_diag = lax.dynamic_slice_in_dim(diag_inverse, col_index * sup_here, sup_here, 0)
    diag, off = [], []
    for chunk, (low, high) in enumerate(chunks):
        product = None
        for step in range(ratio):
            got = gathered[chunk]
            if step:
                got = [send(g, swap(step)) for g in got]
            term = lax.dot_general(
                jnp.concatenate(got, axis=1),
                parts[step],
                (((0,), (1,)), ((), ())),
                preferred_element_type=jnp.float32,
            )
            product = term if product is None else product + term
        product = product.reshape(n_col, -1, rows_here)
        slots = []
        for step in range(n_col):
            slots.append(
                lax.dynamic_index_in_dim(product, plane ^ col_index ^ step, 0, keepdims=False)
            )
        arrived = [send(slots[step].astype(jnp.bfloat16), shift(step)) for step in range(1, n_col)]
        total = slots[0]
        for value in arrived:
            total = total + value.astype(jnp.float32)
        off.append((-total).astype(jnp.bfloat16))
        low_total = total.astype(jnp.bfloat16)
        for sup in range(high - low):
            part_of = slice(sup * width, (sup + 1) * width)
            diag.append(
                lax.dot_general(
                    own[chunk][:, part_of],
                    low_total[part_of],
                    (((0,), (1,)), ((), ())),
                    preferred_element_type=jnp.float32,
                )
            )
    sums = []
    last = chunks[-1][0]
    if last:
        sums.append(exchange(jnp.stack(diag[:last])))
    sums.append(exchange(jnp.stack(diag[last:])))
    done = jnp.concatenate(off, axis=0)
    if not last:
        return done, own_diag + sums[0]
    base = jnp.concatenate([own_diag[:last] + sums[0], own_diag[last:]])
    base = lax.optimization_barrier(base)
    return done, lax.dynamic_update_slice_in_dim(base, base[last:] + sums[1], last, 0)


def split(count):
    edges = list(range(count + 1))
    return list(zip(edges[:-1], edges[1:]))


def solution(mesh):
    return jax.shard_map(
        body,
        mesh=mesh,
        in_specs=(P("row", "col"), P("row", "col"), P(), P()),
        out_specs=(P("col", "row"), P("col", None, None)),
        check_vma=False,
    )
```
